32 devices in a mesh: gx: 4 (over z), gy: 4 (over x, core), gz: 2 (over y).
Axes of the slice: x: 2, y: 2, z: 4, core: 2. Of those that a mesh axis runs over, the one named last changes fastest.
Arguments:
- turbulence: float32 [128, 1024, 1024], P('gz', 'gx', 'gy'), may hold values from -6 to 6
Outputs:
- coefficients: float32 [128, 1024, 1024], P('gz', 'gx', 'gy')
The draws below stay inside these ranges and needn't reach their ends.
All inputs are finite; a program needn't handle non-finite values.
Results may differ from the reference program's by a relative error of at most 0.000075.
Values sent between devices are 32-bit elements; how exact they have to be, the bound alone decides.
No kernel may reach another device: no remote copies, remote signals or barrier semaphores. Data moves between devices by JAX's collectives and lax.ppermute only.
A program may use at most 128 MiB of HBM per device.

```python
import jax
import jax.numpy as jnp
from jax import lax

NX = 1024
NY = 1024
NZ = 128
LEVELS = 3


def steps_of(stream_key, dims, pieces, least, largest):
    def one(axis_at, shards_of):
        draws = jax.random.uniform(jax.random.fold_in(jax.random.fold_in(stream_key, 6), axis_at), (shards_of,), jnp.float32, least / len(pieces), largest / len(pieces))
        return jnp.repeat(jnp.exp(draws), dims[axis_at] // shards_of).reshape((-1,) + (1,) * (len(dims) - axis_at - 1))

    gain = one(*pieces[0])
    for cut in pieces[1:]:
        gain = gain * one(*cut)
    return gain


def noise(stream_key, shape, width, bound, shards=(), dtype=jnp.bfloat16):
    gain = steps_of(stream_key, shape, shards, -0.22, 0.18) if shards else 1.0
    values = jax.random.normal(stream_key, shape, jnp.float32) * width * gain
    return jnp.minimum(jnp.maximum(values, -bound), bound).astype(dtype)


def setup_inputs(seed: int = 0) -> dict:
    keys = jax.random.split(jax.random.key(seed), 2)
    turbulence = noise(keys[0], (NZ, NX, NY), 1.0, 6.0, ((0, 2), (1, 4), (2, 4)), jnp.float32)
    return {"turbulence": turbulence}


lift_alpha = -1.586134342059924
lift_beta = -0.052980118572961
lift_gamma = 0.882911075530934
lift_delta = 0.443506852043971
lift_zeta = 1.149604398860241
inverse_zeta = 1.0 / 1.149604398860241


def join_pairs(even_part, odd_part, direction):
    merged = jnp.stack([even_part, odd_part], axis=direction + 1)
    new_shape = list(even_part.shape)
    new_shape[direction] = new_shape[direction] * 2
    return merged.reshape(new_shape)


def lift_along(values, direction):
    length = values.shape[direction]
    even_part = lax.slice_in_dim(values, 0, length, 2, direction)
    odd_part = lax.slice_in_dim(values, 1, length, 2, direction)

    def shifted_next(operand):
        return jnp.roll(operand, -1, axis=direction)

    def shifted_prev(operand):
        return jnp.roll(operand, 1, axis=direction)

    odd_part = odd_part + lift_alpha * (even_part + shifted_next(even_part))
    even_part = even_part + lift_beta * (shifted_prev(odd_part) + odd_part)
    odd_part = odd_part + lift_gamma * (even_part + shifted_next(even_part))
    even_part = even_part + lift_delta * (shifted_prev(odd_part) + odd_part)
    return join_pairs(even_part * lift_zeta, odd_part * inverse_zeta, direction)


def place_inner(finer, coarse):
    full_shape = finer.shape
    sixfold = finer.reshape(full_shape[0] // 2, 2, full_shape[1] // 2, 2, full_shape[2] // 2, 2)
    inserted = coarse.reshape(full_shape[0] // 2, 1, full_shape[1] // 2, 1, full_shape[2] // 2, 1)
    sixfold = lax.dynamic_update_slice(sixfold, inserted, (0, 0, 0, 0, 0, 0))
    return sixfold.reshape(full_shape)


def reference(turbulence):
    finished_levels = []
    current = turbulence
    for level_index in range(LEVELS):
        for direction in range(3):
            current = lift_along(current, direction)
        finished_levels.append(current)
        current = lax.slice(current, (0, 0, 0), current.shape, (2, 2, 2))
    result = finished_levels[-1]
    for finer in reversed(finished_levels[:-1]):
        result = place_inner(finer, result)
    return result
```

```python
import functools

import jax
import jax.numpy as jnp
import numpy as np
from jax import lax
from jax.experimental import pallas as pl
from jax.experimental.pallas import tpu as pltpu
from jax.sharding import PartitionSpec as P

LEVELS = 3
ALPHA = -1.586134342059924
BETA = -0.052980118572961
GAMMA = 0.882911075530934
DELTA = 0.443506852043971
ZETA = 1.149604398860241
INVERSE_ZETA = 1.0 / 1.149604398860241
LANES = 128


def for_right(s_2, d_2, s_1, d_1):
    return d_1 + ALPHA * s_1, s_1 + BETA * (d_2 + ALPHA * (s_2 + s_1))


def for_left(s_0, d_0, s_1):
    return s_0, s_0 + BETA * (d_0 + ALPHA * (s_0 + s_1))


def lift(s, d, before, after, put):
    n = len(s)
    d1_last = before[0] + ALPHA * s[0]
    s1_last = before[1] + BETA * d1_last
    d2_last = None
    for i in range(n + 1):
        if i < n:
            s_next = s[i + 1] if i + 1 < n else after[0]
            d1 = d[i] + ALPHA * (s[i] + s_next)
            s1 = s[i] + BETA * (d1_last + d1)
        else:
            d1, s1 = None, after[1] + BETA * d1_last
        d2 = d1_last + GAMMA * (s1_last + s1)
        if i > 0:
            put(i - 1, (s1_last + DELTA * (d2_last + d2)) * ZETA, d2 * INVERSE_ZETA)
        d1_last, s1_last, d2_last = d1, s1, d2


def lifting_matrices(length):
    n = length // 2
    basis = np.eye(length + 4)
    s = [basis[2 * i] for i in range(n)]
    d = [basis[2 * i + 1] for i in range(n)]
    out = np.zeros((length + 4, length))

    def put(i, even, odd):
        out[:, 2 * i] = even
        out[:, 2 * i + 1] = odd

    rim = basis[length:]
    lift(s, d, (rim[0], rim[1]), (rim[2], rim[3]), put)
    return out[:length], out[length:]


def halves(a):
    high = a.astype(jnp.bfloat16)
    low = (a - high.astype(jnp.float32)).astype(jnp.bfloat16)
    return high, low


def np_halves(a):
    a = a.astype(np.float32)
    high = a.astype(jnp.bfloat16)
    low = (a - high.astype(np.float32)).astype(jnp.bfloat16)
    return high, low


class Sizes:
    def __init__(self, shape, step, valid):
        self.z, self.x, self.lanes = shape
        self.step = step
        self.y = valid
        self.out = max(LANES, -(-valid // LANES) * LANES)
        inner, rim = lifting_matrices(valid)
        full = np.zeros((self.lanes, self.out))
        full[: step * valid : step, :valid] = inner
        self.high, self.low = np_halves(full)
        edge = np.zeros((4, self.out))
        edge[:, :valid] = rim
        self.rim = edge.astype(np.float32)
        rim_high, rim_low = np_halves(edge)
        zeros = np.zeros((4, self.out), rim_high.dtype)
        self.rim_packed = np.concatenate([rim_high, rim_high, rim_low, zeros])


def dot(a, b):
    return jnp.dot(a, b, preferred_element_type=jnp.float32)


def times(rows, high_ref, low_ref):
    a, b = halves(rows)
    return dot(a, high_ref[...]) + dot(b, high_ref[...]) + dot(a, low_ref[...])


def whole(shape):
    return pl.BlockSpec(shape, lambda *_: (0,) * len(shape))


def edges_kernel(sizes, count, x_ref, left_ref, right_ref):
    step, n = sizes.step, sizes.y
    tile = (step * (n - 1)) // LANES * LANES
    low_lane = lax.broadcasted_iota(jnp.int32, (sizes.x, LANES), 1) < LANES // 2
    for p in range(count):
        both = x_ref[p, :, :LANES]
        if tile:
            both = jnp.where(low_lane, both, x_ref[p, :, tile : tile + LANES])
        both = both.T
        f = [both[step * k : step * k + 1] for k in range(3)]
        l = [both[step * (n - k) - tile : step * (n - k) - tile + 1] for k in (4, 3, 2, 1)]
        s, c = for_left(f[0], f[1], f[2])
        a, b = for_right(*l)
        left_ref[p, 0:1] = s
        left_ref[p, 1:2] = c
        right_ref[p, 0:1] = a
        right_ref[p, 1:2] = b


def edges(sizes, x):
    count = min(8, sizes.z)
    out = jax.ShapeDtypeStruct((sizes.z, 2, sizes.x), jnp.float32)
    spec = pl.BlockSpec((count, 2, sizes.x), lambda i: (i, 0, 0))
    return pl.pallas_call(
        functools.partial(edges_kernel, sizes, count),
        grid=(sizes.z // count,),
        in_specs=[pl.BlockSpec((count, sizes.x, sizes.lanes), lambda i: (i, 0, 0))],
        out_specs=[spec, spec],
        out_shape=[out, out],
        name="edges",
    )(x)


def rows_kernel(sizes, top_ref, bottom_ref, rim_rows_ref, high_ref, low_ref, rim_ref, left_ref, right_ref):
    z = sizes.z

    def across(ref, at):
        out = times(ref[...].reshape(z * 8, sizes.lanes), high_ref, low_ref)
        for h in range(4):
            column = rim_rows_ref[:, 8 * at : 8 * at + 8, h : h + 1].reshape(z * 8, 1)
            out = out + column * rim_ref[h : h + 1]
        return out.reshape(z, 8, sizes.out)

    top = across(top_ref, 0)
    bottom = across(bottom_ref, 1)
    s, c = for_left(top[:, 0:1], top[:, 1:2], top[:, 2:3])
    a, b = for_right(bottom[:, 4:5], bottom[:, 5:6], bottom[:, 6:7], bottom[:, 7:8])
    left_ref[:, 0:1] = s
    left_ref[:, 1:2] = c
    right_ref[:, 0:1] = a
    right_ref[:, 1:2] = b


def rows(sizes, x, rim_rows):
    z = sizes.z
    out = jax.ShapeDtypeStruct((z, 2, sizes.out), jnp.float32)
    last = sizes.x // 8 - 1
    return pl.pallas_call(
        functools.partial(rows_kernel, sizes),
        grid=(1,),
        in_specs=[
            pl.BlockSpec((z, 8, sizes.lanes), lambda i: (0, 0, 0)),
            pl.BlockSpec((z, 8, sizes.lanes), lambda i: (0, last, 0)),
            whole(rim_rows.shape),
            whole(sizes.high.shape),
            whole(sizes.low.shape),
            whole(sizes.rim.shape),
        ],
        out_specs=[whole(out.shape), whole(out.shape)],
        out_shape=[out, out],
        name="rows",
    )(x, x, rim_rows, sizes.high, sizes.low, sizes.rim)


def across_planes(sizes, count, refs, work):
    x_ref, yb_ref, ya_ref, xb_ref, xa_ref, high_ref, low_ref, rim_ref = refs
    n = sizes.x // 2
    at = lax.broadcasted_iota(jnp.int32, (n, LANES), 0)

    def shifted_next(v, edge):
        return jnp.where(at == n - 1, edge, pltpu.roll(v, n - 1, 0))

    def shifted_prev(v, edge):
        return jnp.where(at == 0, edge, pltpu.roll(v, 1, 0))

    for p in range(count):
        rim = jnp.concatenate([yb_ref[p], ya_ref[p]], axis=0)
        high = rim.astype(jnp.bfloat16).astype(jnp.float32)
        packed = jnp.concatenate([high, rim - high, high, jnp.zeros_like(high)], axis=0)
        across = times(x_ref[p], high_ref, low_ref) + dot(packed.T.astype(jnp.bfloat16), rim_ref[...])
        for c in range(sizes.out // LANES):
            lanes = slice(c * LANES, (c + 1) * LANES)
            work[p, c] = across[:, lanes]
            s = work[p, c, pl.ds(0, n, stride=2), :]
            d = work[p, c, pl.ds(1, n, stride=2), :]
            a, b = xb_ref[p, 0:1, lanes], xb_ref[p, 1:2, lanes]
            s_n, c_n = xa_ref[p, 0:1, lanes], xa_ref[p, 1:2, lanes]
            d1 = d + ALPHA * (s + shifted_next(s, s_n))
            d1_b = a + ALPHA * s[0:1]
            s1 = s + BETA * (shifted_prev(d1, d1_b) + d1)
            s1_b = b + BETA * d1_b
            s1_a = c_n + BETA * d1[n - 1 : n]
            d2 = d1 + GAMMA * (s1 + shifted_next(s1, s1_a))
            d2_b = d1_b + GAMMA * (s1_b + s1[0:1])
            s2 = s1 + DELTA * (shifted_prev(d2, d2_b) + d2)
            work[p, c, pl.ds(0, n, stride=2), :] = s2 * ZETA
            work[p, c, pl.ds(1, n, stride=2), :] = d2 * INVERSE_ZETA


def ends_kernel(sizes, *args):
    refs, left_ref, right_ref, work = args[:8], args[8], args[9], args[10]
    across_planes(sizes, 4, refs, work)
    for c in range(sizes.out // LANES):
        lanes = slice(c * LANES, (c + 1) * LANES)
        v = [work[p, c] for p in range(4)]

        @pl.when(pl.program_id(0) == 0)
        def _():
            left_ref[0, :, lanes], left_ref[1, :, lanes] = for_left(*v[:3])

        @pl.when(pl.program_id(0) == 1)
        def _():
            right_ref[0, :, lanes], right_ref[1, :, lanes] = for_right(*v)


def stream_kernel(sizes, steps, more, *args):
    refs, out_ref = args[:8], args[8]
    next_ref = args[9] if more else None
    work, state = args[-2:]
    step = pl.program_id(0)
    nx = sizes.x
    chunk = min(32, nx)

    @pl.when(step == 0)
    def _():
        state[...] = jnp.zeros_like(state)

    @pl.when(step < steps)
    def _():
        across_planes(sizes, 4, refs, work)

    @pl.when(step == steps)
    def _():
        work[...] = jnp.zeros_like(work)

    for c in range(sizes.out // LANES):
        lanes = slice(c * LANES, (c + 1) * LANES)
        for r in range(nx // chunk):
            at = slice(r * chunk, (r + 1) * chunk)
            s, d, d1_b, s1_b, d2_b = (state[k, c, at] for k in range(5))
            for q in range(2):
                s_n, d_n = work[2 * q, c, at], work[2 * q + 1, c, at]
                d1 = d + ALPHA * (s + s_n)
                s1 = s + BETA * (d1_b + d1)
                d2 = d1_b + GAMMA * (s1_b + s1)
                even = (s1_b + DELTA * (d2_b + d2)) * ZETA
                out_ref[2 * q, at, lanes] = even
                out_ref[2 * q + 1, at, lanes] = d2 * INVERSE_ZETA
                if more:
                    work[2 * q, c, at] = even
                s, d, d1_b, s1_b, d2_b = s_n, d_n, d1, s1, d2
            for k, v in enumerate((s, d, d1_b, s1_b, d2_b)):
                state[k, c, at] = v
        if more:
            for q in range(2):
                next_ref[q, :, lanes] = work[2 * q, c, pl.ds(0, nx // 2, stride=2), :]


def across_specs(sizes, place):
    return [
        pl.BlockSpec((4, sizes.x, sizes.lanes), place),
        pl.BlockSpec((4, 2, sizes.x), place),
        pl.BlockSpec((4, 2, sizes.x), place),
        pl.BlockSpec((4, 2, sizes.out), place),
        pl.BlockSpec((4, 2, sizes.out), place),
        whole(sizes.high.shape),
        whole(sizes.low.shape),
        whole(sizes.rim_packed.shape),
    ]


def cost(sizes, count):
    return pl.CostEstimate(
        flops=count * sizes.x * sizes.out * sizes.lanes * 8,
        bytes_accessed=count * sizes.x * (sizes.out + sizes.lanes) * 4,
        transcendentals=0,
    )


def ends(sizes, *operands):
    out = jax.ShapeDtypeStruct((2, sizes.x, sizes.out), jnp.float32)
    last = sizes.z // 4 - 1
    return pl.pallas_call(
        functools.partial(ends_kernel, sizes),
        grid=(2,),
        in_specs=across_specs(sizes, lambda i: (i * last, 0, 0)),
        out_specs=[whole(out.shape), whole(out.shape)],
        out_shape=[out, out],
        scratch_shapes=[pltpu.VMEM((4, sizes.out // LANES, sizes.x, LANES), jnp.float32)],
        cost_estimate=cost(sizes, 8),
        name="ends",
    )(*operands, sizes.high, sizes.low, sizes.rim_packed)


def stream(sizes, more, *operands):
    z, nx, width = sizes.z, sizes.x, sizes.out
    steps = z // 4
    behind = lambda i: (jnp.maximum(i - 1, 0), 0, 0)
    out_shape = [jax.ShapeDtypeStruct((z, nx, width), jnp.float32)]
    out_specs = [pl.BlockSpec((4, nx, width), behind)]
    if more:
        out_shape.append(jax.ShapeDtypeStruct((z // 2, nx // 2, width), jnp.float32))
        out_specs.append(pl.BlockSpec((2, nx // 2, width), behind))
    return pl.pallas_call(
        functools.partial(stream_kernel, sizes, steps, more),
        grid=(steps + 1,),
        in_specs=across_specs(sizes, lambda i: (jnp.minimum(i, steps - 1), 0, 0)),
        out_specs=out_specs,
        out_shape=out_shape,
        scratch_shapes=[
            pltpu.VMEM((4, width // LANES, nx, LANES), jnp.float32),
            pltpu.VMEM((5, width // LANES, nx, LANES), jnp.float32),
        ],
        cost_estimate=cost(sizes, z),
        name="stream",
    )(*operands, sizes.high, sizes.low, sizes.rim_packed)


def finish_kernel(sizes, more, zb_ref, za_ref, t_ref, *rest):
    if more:
        _, out_ref, next_ref, work = rest
    else:
        out_ref = rest[0]
    nx = sizes.x
    rim = lifting_matrices(sizes.z)[1]
    single = sizes.z == 4

    def apply(sides):
        for k in range(4):
            for c in range(sizes.out // LANES):
                lanes = slice(c * LANES, (c + 1) * LANES)
                total = t_ref[k, :, lanes]
                for h in range(4):
                    factor = rim[h, k if h < 2 else sizes.z - 4 + k]
                    if factor != 0.0 and h // 2 in sides:
                        ref = (zb_ref, za_ref)[h // 2]
                        total = total + float(factor) * ref[h % 2, :, lanes]
                out_ref[k, :, lanes] = total
                if more and k % 2 == 0:
                    work[c] = total
                    next_ref[k // 2, :, lanes] = work[c, pl.ds(0, nx // 2, stride=2), :]

    if single:
        apply((0, 1))
    else:
        pl.when(pl.program_id(0) == 0)(lambda: apply((0,)))
        pl.when(pl.program_id(0) == 1)(lambda: apply((1,)))


def finish(sizes, made, z_before, z_after):
    more = len(made) == 2
    z, nx, width = sizes.z, sizes.x, sizes.out
    last = z // 4 - 1
    place = lambda i: (i * last, 0, 0)
    specs = [pl.BlockSpec((4, nx, width), place)]
    scratch = []
    if more:
        specs.append(pl.BlockSpec((2, nx // 2, width), place))
        scratch.append(pltpu.VMEM((width // LANES, nx, LANES), jnp.float32))
    return pl.pallas_call(
        functools.partial(finish_kernel, sizes, more),
        grid=(min(2, last + 1),),
        in_specs=[whole((2, nx, width)), whole((2, nx, width))] + specs,
        out_specs=specs,
        out_shape=[jax.ShapeDtypeStruct(m.shape, m.dtype) for m in made],
        input_output_aliases={2 + k: k for k in range(len(made))},
        scratch_shapes=scratch,
        name="finish",
    )(z_before, z_after, *made)


def place_kernel(count, t_ref, r_ref, spread_ref, out_ref, work):
    nx, width = t_ref.shape[2], t_ref.shape[3]
    n = nx // 2
    even_lane = lax.broadcasted_iota(jnp.int32, (n, LANES), 1) % 2 == 0
    for p in range(count):
        rest = r_ref[p]
        high = rest.astype(jnp.bfloat16)
        rest = rest - high.astype(jnp.float32)
        middle, low = halves(rest)
        table = spread_ref[...]
        spread = dot(high, table) + dot(middle, table) + dot(low, table)
        for c in range(width // LANES):
            lanes = slice(c * LANES, (c + 1) * LANES)
            work[c] = t_ref[p, 0, :, lanes]
            even_rows = work[c, pl.ds(0, n, stride=2), :]
            work[c, pl.ds(0, n, stride=2), :] = jnp.where(even_lane, spread[:, lanes], even_rows)
            out_ref[p, 0, :, lanes] = work[c]


def place(t, r):
    z, nx, width = t.shape
    table = np.zeros((r.shape[2], width), np.float32)
    for j in range(min(r.shape[2], width // 2)):
        table[j, 2 * j] = 1.0
    count = min(8, z // 2)
    spec = pl.BlockSpec((count, 1, nx, width), lambda i: (i, 0, 0, 0))
    paired = t.reshape(z // 2, 2, nx, width)
    return pl.pallas_call(
        functools.partial(place_kernel, count),
        grid=(z // 2 // count,),
        in_specs=[
            spec,
            pl.BlockSpec((count,) + r.shape[1:], lambda i: (i, 0, 0)),
            whole(table.shape),
        ],
        out_specs=spec,
        out_shape=jax.ShapeDtypeStruct(paired.shape, jnp.float32),
        input_output_aliases={0: 0},
        scratch_shapes=[pltpu.VMEM((width // LANES, nx, LANES), jnp.float32)],
        name="place",
    )(paired, r, table.astype(jnp.bfloat16)).reshape(t.shape)


def exchange(axis, left, right):
    count = lax.axis_size(axis)
    before = lax.ppermute(right, axis, [(i, (i + 1) % count) for i in range(count)])
    after = lax.ppermute(left, axis, [(i, (i - 1) % count) for i in range(count)])
    return before, after


def level(sizes, x, more):
    y_before, y_after = exchange("gy", *edges(sizes, x))
    rim = jnp.concatenate([y_before, y_after], axis=1)
    rim_rows = jnp.concatenate([rim[:, :, :8], rim[:, :, -8:]], axis=2).swapaxes(1, 2)
    x_before, x_after = exchange("gx", *rows(sizes, x, rim_rows))
    sides = (y_before, y_after, x_before, x_after)
    z_before, z_after = exchange("gz", *ends(sizes, x, *sides))
    return finish(sizes, stream(sizes, more, x, *sides), z_before, z_after)


def local(turbulence):
    valid = turbulence.shape[2]
    current, step, done = turbulence, 1, []
    for index in range(LEVELS):
        more = index + 1 < LEVELS
        sizes = Sizes(current.shape, step, valid)
        made = level(sizes, current, more)
        done.append(made[0])
        if more:
            current, step, valid = made[1], 2, valid // 2
    result = done[-1]
    for finer in reversed(done[:-1]):
        result = place(finer, result)
    return result[:, :, : turbulence.shape[2]]


def solution(mesh):
    spec = P("gz", "gx", "gy")
    return jax.shard_map(local, mesh=mesh, in_specs=(spec,), out_specs=spec, check_vma=False)
```

```python
import functools

import jax
import jax.numpy as jnp
import numpy as np
from jax import lax
from jax.experimental import pallas as pl
from jax.experimental.pallas import tpu as pltpu
from jax.sharding import PartitionSpec as P

LEVELS = 3
ALPHA = -1.586134342059924
BETA = -0.052980118572961
GAMMA = 0.882911075530934
DELTA = 0.443506852043971
ZETA = 1.149604398860241
INVERSE_ZETA = 1.0 / 1.149604398860241
LANES = 128
EDGE = 8


def for_right(s_2, d_2, s_1, d_1):
    return d_1 + ALPHA * s_1, s_1 + BETA * (d_2 + ALPHA * (s_2 + s_1))


def for_left(s_0, d_0, s_1):
    return s_0, s_0 + BETA * (d_0 + ALPHA * (s_0 + s_1))


def lift(s, d, before, after, put):
    n = len(s)
    d1_last = before[0] + ALPHA * s[0]
    s1_last = before[1] + BETA * d1_last
    d2_last = None
    for i in range(n + 1):
        if i < n:
            s_next = s[i + 1] if i + 1 < n else after[0]
            d1 = d[i] + ALPHA * (s[i] + s_next)
            s1 = s[i] + BETA * (d1_last + d1)
        else:
            d1, s1 = None, after[1] + BETA * d1_last
        d2 = d1_last + GAMMA * (s1_last + s1)
        if i > 0:
            put(i - 1, (s1_last + DELTA * (d2_last + d2)) * ZETA, d2 * INVERSE_ZETA)
        d1_last, s1_last, d2_last = d1, s1, d2


def lifting_matrices(length):
    n = length // 2
    basis = np.eye(length + 4)
    s = [basis[2 * i] for i in range(n)]
    d = [basis[2 * i + 1] for i in range(n)]
    out = np.zeros((length + 4, length))

    def put(i, even, odd):
        out[:, 2 * i] = even
        out[:, 2 * i + 1] = odd

    rim = basis[length:]
    lift(s, d, (rim[0], rim[1]), (rim[2], rim[3]), put)
    return out[:length], out[length:]


def halves(a):
    high = a.astype(jnp.bfloat16)
    low = (a - high.astype(jnp.float32)).astype(jnp.bfloat16)
    return high, low


def np_halves(a):
    a = a.astype(np.float32)
    high = a.astype(jnp.bfloat16)
    low = (a - high.astype(np.float32)).astype(jnp.bfloat16)
    return high, low


class Sizes:
    def __init__(self, shape, step, valid):
        self.z, self.x, self.lanes = shape
        self.step = step
        self.y = valid
        self.out = max(LANES, -(-valid // LANES) * LANES)
        inner, rim = lifting_matrices(valid)
        full = np.zeros((self.lanes, self.out))
        full[: step * valid : step, :valid] = inner
        self.high, self.low = np_halves(full)
        edge = np.zeros((4, self.out))
        edge[:, :valid] = rim
        self.rim = edge.astype(np.float32)
        rim_high, rim_low = np_halves(edge)
        zeros = np.zeros((4, self.out), rim_high.dtype)
        self.rim_packed = np.concatenate([rim_high, rim_high, rim_low, zeros])


def dot(a, b):
    return jnp.dot(a, b, preferred_element_type=jnp.float32)


def times(rows, high_ref, low_ref):
    a, b = halves(rows)
    return dot(a, high_ref[...]) + dot(b, high_ref[...]) + dot(a, low_ref[...])


def whole(shape):
    return pl.BlockSpec(shape, lambda *_: (0,) * len(shape))


def edges_kernel(sizes, count, x_ref, left_ref, right_ref):
    step, n = sizes.step, sizes.y
    tile = (step * (n - 1)) // LANES * LANES
    low_lane = lax.broadcasted_iota(jnp.int32, (sizes.x, LANES), 1) < LANES // 2
    for p in range(count):
        both = x_ref[p, :, :LANES]
        if tile:
            both = jnp.where(low_lane, both, x_ref[p, :, tile : tile + LANES])
        both = both.T
        f = [both[step * k : step * k + 1] for k in range(3)]
        l = [both[step * (n - k) - tile : step * (n - k) - tile + 1] for k in (4, 3, 2, 1)]
        s, c = for_left(f[0], f[1], f[2])
        a, b = for_right(*l)
        left_ref[p, 0:1] = s
        left_ref[p, 1:2] = c
        right_ref[p, 0:1] = a
        right_ref[p, 1:2] = b


def edges(sizes, x):
    count = min(16, sizes.z)
    out = jax.ShapeDtypeStruct((sizes.z, 2, sizes.x), jnp.float32)
    spec = pl.BlockSpec((count, 2, sizes.x), lambda i: (i, 0, 0))
    return pl.pallas_call(
        functools.partial(edges_kernel, sizes, count),
        grid=(sizes.z // count,),
        in_specs=[pl.BlockSpec((count, sizes.x, sizes.lanes), lambda i: (i, 0, 0))],
        out_specs=[spec, spec],
        out_shape=[out, out],
        name="edges",
    )(x)


def rows_kernel(sizes, top_ref, bottom_ref, rim_rows_ref, high_ref, low_ref, rim_ref, left_ref, right_ref):
    z = sizes.z

    def across(ref, at):
        out = times(ref[...].reshape(z * 8, sizes.lanes), high_ref, low_ref)
        for h in range(4):
            column = rim_rows_ref[:, 8 * at : 8 * at + 8, h : h + 1].reshape(z * 8, 1)
            out = out + column * rim_ref[h : h + 1]
        return out.reshape(z, 8, sizes.out)

    top = across(top_ref, 0)
    bottom = across(bottom_ref, 1)
    s, c = for_left(top[:, 0:1], top[:, 1:2], top[:, 2:3])
    a, b = for_right(bottom[:, 4:5], bottom[:, 5:6], bottom[:, 6:7], bottom[:, 7:8])
    left_ref[:, 0:1] = s
    left_ref[:, 1:2] = c
    right_ref[:, 0:1] = a
    right_ref[:, 1:2] = b


def rows(sizes, x, rim_rows):
    z = sizes.z
    out = jax.ShapeDtypeStruct((z, 2, sizes.out), jnp.float32)
    last = sizes.x // 8 - 1
    return pl.pallas_call(
        functools.partial(rows_kernel, sizes),
        grid=(1,),
        in_specs=[
            pl.BlockSpec((z, 8, sizes.lanes), lambda i: (0, 0, 0)),
            pl.BlockSpec((z, 8, sizes.lanes), lambda i: (0, last, 0)),
            whole(rim_rows.shape),
            whole(sizes.high.shape),
            whole(sizes.low.shape),
            whole(sizes.rim.shape),
        ],
        out_specs=[whole(out.shape), whole(out.shape)],
        out_shape=[out, out],
        name="rows",
    )(x, x, rim_rows, sizes.high, sizes.low, sizes.rim)


def across_planes(sizes, count, refs, work):
    x_ref, yb_ref, ya_ref, xb_ref, xa_ref, high_ref, low_ref, rim_ref = refs
    nx = sizes.x
    n = nx // 2
    for p in range(count):
        rim = jnp.concatenate([yb_ref[p], ya_ref[p]], axis=0)
        high = rim.astype(jnp.bfloat16).astype(jnp.float32)
        packed = jnp.concatenate([high, rim - high, high, jnp.zeros_like(high)], axis=0)
        across = times(x_ref[p], high_ref, low_ref) + dot(packed.T.astype(jnp.bfloat16), rim_ref[...])
        for c in range(sizes.out // LANES):
            lanes = slice(c * LANES, (c + 1) * LANES)

            def row(ref, k):
                return ref[p, k : k + 1, lanes]

            def at(start):
                return pl.ds(EDGE + start, n, stride=2)

            def one(k):
                return slice(EDGE + k, EDGE + k + 1)

            work[p, c, EDGE : EDGE + nx] = across[:, lanes]
            work[p, c, one(nx)] = row(xa_ref, 0)
            s = work[p, c, at(0)]
            d1 = work[p, c, at(1)] + ALPHA * (s + work[p, c, at(2)])
            d1_b = row(xb_ref, 0) + ALPHA * s[0:1]
            work[p, c, at(1)] = d1
            work[p, c, one(-1)] = d1_b
            s1 = s + BETA * (work[p, c, at(-1)] + d1)
            s1_b = row(xb_ref, 1) + BETA * d1_b
            work[p, c, at(0)] = s1
            work[p, c, one(nx)] = row(xa_ref, 1) + BETA * d1[n - 1 : n]
            d2 = d1 + GAMMA * (s1 + work[p, c, at(2)])
            work[p, c, at(1)] = d2
            work[p, c, one(-1)] = d1_b + GAMMA * (s1_b + s1[0:1])
            work[p, c, at(0)] = s1 + DELTA * (work[p, c, at(-1)] + d2)


def x_scale(height):
    even = lax.broadcasted_iota(jnp.int32, (height, LANES), 0) % 2 == 0
    return jnp.where(even, ZETA, INVERSE_ZETA).astype(jnp.float32)


def ends_kernel(sizes, *args):
    refs, out_ref, work = args[:8], args[8], args[9]
    across_planes(sizes, 4, refs, work)
    for c in range(sizes.out // LANES):
        lanes = slice(c * LANES, (c + 1) * LANES)
        v = [work[p, c, EDGE : EDGE + sizes.x] for p in range(4)]

        @pl.when(pl.program_id(0) == 0)
        def _():
            out_ref[0, :, lanes], out_ref[1, :, lanes] = for_left(*v[:3])

        @pl.when(pl.program_id(0) == 1)
        def _():
            out_ref[2, :, lanes], out_ref[3, :, lanes] = for_right(*v)


def stream_kernel(sizes, group, steps, more, *args):
    refs, out_ref = args[:8], args[8]
    next_ref = args[9] if more else None
    work, state = args[-2:]
    step = pl.program_id(0)
    nx = sizes.x
    chunk = min(32, nx)
    even_scale = x_scale(chunk) * ZETA
    odd_scale = x_scale(chunk) * INVERSE_ZETA

    def take(pairs, slot):
        for c in range(sizes.out // LANES):
            lanes = slice(c * LANES, (c + 1) * LANES)
            for r in range(nx // chunk):
                at = slice(r * chunk, (r + 1) * chunk)
                held = slice(EDGE + r * chunk, EDGE + (r + 1) * chunk)
                s, d, d1_b, s1_b, d2_b = (state[k, c, at] for k in range(5))
                for q, pair in enumerate(pairs, slot):
                    s_n, d_n = work[2 * pair, c, held], work[2 * pair + 1, c, held]
                    d1 = d + ALPHA * (s + s_n)
                    s1 = s + BETA * (d1_b + d1)
                    d2 = d1_b + GAMMA * (s1_b + s1)
                    even = (s1_b + DELTA * (d2_b + d2)) * even_scale
                    out_ref[2 * q, at, lanes] = even
                    out_ref[2 * q + 1, at, lanes] = d2 * odd_scale
                    if more:
                        work[2 * pair, c, held] = even
                    s, d, d1_b, s1_b, d2_b = s_n, d_n, d1, s1, d2
                for k, v in enumerate((s, d, d1_b, s1_b, d2_b)):
                    state[k, c, at] = v
            if more:
                for q, pair in enumerate(pairs, slot):
                    next_ref[q, :, lanes] = work[2 * pair, c, pl.ds(EDGE, nx // 2, stride=2), :]

    late = range(2, group // 2)

    @pl.when(step == 0)
    def _():
        state[...] = jnp.zeros_like(state)
        work[...] = jnp.zeros_like(work)

    @pl.when(step < steps)
    def _():
        take(late, 0)
        across_planes(sizes, group, refs, work)

    @pl.when(step == steps)
    def _():
        take(late, 0)
        work[:4] = jnp.zeros((4,) + work.shape[1:], jnp.float32)

    take(range(2), len(late))


def across_specs(sizes, count, place):
    return [
        pl.BlockSpec((count, sizes.x, sizes.lanes), place),
        pl.BlockSpec((count, 2, sizes.x), place),
        pl.BlockSpec((count, 2, sizes.x), place),
        pl.BlockSpec((count, 2, sizes.out), place),
        pl.BlockSpec((count, 2, sizes.out), place),
        whole(sizes.high.shape),
        whole(sizes.low.shape),
        whole(sizes.rim_packed.shape),
    ]


def cost(sizes, count):
    return pl.CostEstimate(
        flops=count * sizes.x * sizes.out * sizes.lanes * 8,
        bytes_accessed=count * sizes.x * (sizes.out + sizes.lanes) * 4,
        transcendentals=0,
    )


def ends(sizes, *operands):
    out = jax.ShapeDtypeStruct((4, sizes.x, sizes.out), jnp.float32)
    last = sizes.z // 4 - 1
    return pl.pallas_call(
        functools.partial(ends_kernel, sizes),
        grid=(2,),
        in_specs=across_specs(sizes, 4, lambda i: (i * last, 0, 0)),
        out_specs=whole(out.shape),
        out_shape=out,
        scratch_shapes=[pltpu.VMEM((4, sizes.out // LANES, sizes.x + 2 * EDGE, LANES), jnp.float32)],
        cost_estimate=cost(sizes, 8),
        name="ends",
    )(*operands, sizes.high, sizes.low, sizes.rim_packed)


def stream(sizes, more, *operands):
    z, nx, width = sizes.z, sizes.x, sizes.out
    group = min(8, z)
    steps = z // group
    behind = lambda i: (jnp.maximum(i - 1, 0), 0, 0)
    out_shape = [jax.ShapeDtypeStruct((z, nx, width), jnp.float32)]
    out_specs = [pl.BlockSpec((group, nx, width), behind)]
    if more:
        out_shape.append(jax.ShapeDtypeStruct((z // 2, nx // 2, width), jnp.float32))
        out_specs.append(pl.BlockSpec((group // 2, nx // 2, width), behind))
    return pl.pallas_call(
        functools.partial(stream_kernel, sizes, group, steps, more),
        grid=(steps + 1,),
        in_specs=across_specs(sizes, group, lambda i: (jnp.minimum(i, steps - 1), 0, 0)),
        out_specs=out_specs,
        out_shape=out_shape,
        scratch_shapes=[
            pltpu.VMEM((group, width // LANES, nx + 2 * EDGE, LANES), jnp.float32),
            pltpu.VMEM((5, width // LANES, nx, LANES), jnp.float32),
        ],
        cost_estimate=cost(sizes, z),
        name="stream",
    )(*operands, sizes.high, sizes.low, sizes.rim_packed)


def finish_kernel(sizes, more, z_ref, t_ref, *rest):
    if more:
        _, out_ref, next_ref, work = rest
    else:
        out_ref = rest[0]
    nx = sizes.x
    rim = lifting_matrices(sizes.z)[1]
    single = sizes.z == 4
    scale = x_scale(nx)

    def apply(sides):
        for k in range(4):
            for c in range(sizes.out // LANES):
                lanes = slice(c * LANES, (c + 1) * LANES)
                total = jnp.zeros((nx, LANES), jnp.float32)
                for h in range(4):
                    factor = rim[h, k if h < 2 else sizes.z - 4 + k]
                    if factor != 0.0 and h // 2 in sides:
                        total = total + float(factor) * z_ref[(h + 2) % 4, :, lanes]
                total = t_ref[k, :, lanes] + scale * total
                out_ref[k, :, lanes] = total
                if more and k % 2 == 0:
                    work[c] = total
                    next_ref[k // 2, :, lanes] = work[c, pl.ds(0, nx // 2, stride=2), :]

    if single:
        apply((0, 1))
    else:
        pl.when(pl.program_id(0) == 0)(lambda: apply((0,)))
        pl.when(pl.program_id(0) == 1)(lambda: apply((1,)))


def finish(sizes, made, z_planes):
    more = len(made) == 2
    z, nx, width = sizes.z, sizes.x, sizes.out
    last = z // 4 - 1
    place = lambda i: (i * last, 0, 0)
    specs = [pl.BlockSpec((4, nx, width), place)]
    scratch = []
    if more:
        specs.append(pl.BlockSpec((2, nx // 2, width), place))
        scratch.append(pltpu.VMEM((width // LANES, nx, LANES), jnp.float32))
    return pl.pallas_call(
        functools.partial(finish_kernel, sizes, more),
        grid=(min(2, last + 1),),
        in_specs=[whole((4, nx, width))] + specs,
        out_specs=specs,
        out_shape=[jax.ShapeDtypeStruct(m.shape, m.dtype) for m in made],
        input_output_aliases={1 + k: k for k in range(len(made))},
        scratch_shapes=scratch,
        name="finish",
    )(z_planes, *made)


def spread_lanes(rows, table):
    high = rows.astype(jnp.bfloat16)
    middle, low = halves(rows - high.astype(jnp.float32))
    return dot(high, table) + dot(middle, table) + dot(low, table)


def put_inner(plane, inner, table, work):
    nx, width = plane.shape
    n = nx // 2
    even_lane = lax.broadcasted_iota(jnp.int32, (n, LANES), 1) % 2 == 0
    spread = spread_lanes(inner, table)
    for c in range(width // LANES):
        lanes = slice(c * LANES, (c + 1) * LANES)
        work[c] = plane[:, lanes]
        even_rows = work[c, pl.ds(0, n, stride=2), :]
        work[c, pl.ds(0, n, stride=2), :] = jnp.where(even_lane, spread[:, lanes], even_rows)


def place_kernel(count, t_ref, middle_ref, inner_ref, outer_table_ref, inner_table_ref, out_ref, work, inner_work):
    width, middle_width = t_ref.shape[3], middle_ref.shape[2]
    for p in range(count):
        middle = middle_ref[p]
        if p % 2 == 0:
            put_inner(middle, inner_ref[p // 2], inner_table_ref[...], inner_work)
            middle = jnp.concatenate([inner_work[c] for c in range(middle_width // LANES)], axis=1)
        put_inner(t_ref[p, 0], middle, outer_table_ref[...], work)
        for c in range(width // LANES):
            out_ref[p, 0, :, c * LANES : (c + 1) * LANES] = work[c]


def spread_table(inner, outer):
    table = np.zeros((inner, outer), np.float32)
    for j in range(min(inner, outer // 2)):
        table[j, 2 * j] = 1.0
    return table.astype(jnp.bfloat16)


def place(t, middle, inner):
    z, nx, width = t.shape
    tables = spread_table(middle.shape[2], width), spread_table(inner.shape[2], middle.shape[2])
    count = min(8, z // 2)
    spec = pl.BlockSpec((count, 1, nx, width), lambda i: (i, 0, 0, 0))
    paired = t.reshape(z // 2, 2, nx, width)
    return pl.pallas_call(
        functools.partial(place_kernel, count),
        grid=(z // 2 // count,),
        in_specs=[
            spec,
            pl.BlockSpec((count,) + middle.shape[1:], lambda i: (i, 0, 0)),
            pl.BlockSpec((count // 2,) + inner.shape[1:], lambda i: (i, 0, 0)),
            whole(tables[0].shape),
            whole(tables[1].shape),
        ],
        out_specs=spec,
        out_shape=jax.ShapeDtypeStruct(paired.shape, jnp.float32),
        input_output_aliases={0: 0},
        scratch_shapes=[
            pltpu.VMEM((width // LANES, nx, LANES), jnp.float32),
            pltpu.VMEM((middle.shape[2] // LANES,) + middle.shape[1:2] + (LANES,), jnp.float32),
        ],
        name="place",
    )(paired, middle, inner, *tables).reshape(t.shape)


def exchange(axis, left, right):
    count = lax.axis_size(axis)
    before = lax.ppermute(right, axis, [(i, (i + 1) % count) for i in range(count)])
    after = lax.ppermute(left, axis, [(i, (i - 1) % count) for i in range(count)])
    return before, after


def exchange_z(planes):
    count = lax.axis_size("gz")
    if count == 2:
        return lax.ppermute(planes, "gz", [(0, 1), (1, 0)])
    before, after = exchange("gz", planes[:2], planes[2:])
    return jnp.concatenate([after, before])


def level(sizes, x, more):
    y_before, y_after = exchange("gy", *edges(sizes, x))
    rim = jnp.concatenate([y_before, y_after], axis=1)
    rim_rows = jnp.concatenate([rim[:, :, :8], rim[:, :, -8:]], axis=2).swapaxes(1, 2)
    x_before, x_after = exchange("gx", *rows(sizes, x, rim_rows))
    operands = (x, y_before, y_after, x_before, x_after)
    z_planes = exchange_z(ends(sizes, *operands))
    return finish(sizes, stream(sizes, more, *operands), z_planes)


def local(turbulence):
    valid = turbulence.shape[2]
    current, step, done = turbulence, 1, []
    for index in range(LEVELS):
        more = index + 1 < LEVELS
        sizes = Sizes(current.shape, step, valid)
        made = level(sizes, current, more)
        done.append(made[0])
        if more:
            current, step, valid = made[1], 2, valid // 2
    return place(*done)[:, :, : turbulence.shape[2]]


def solution(mesh):
    spec = P("gz", "gx", "gy")
    return jax.shard_map(local, mesh=mesh, in_specs=(spec,), out_specs=spec, check_vma=False)
```

```python
import functools

import jax
import jax.numpy as jnp
import numpy as np
from jax import lax
from jax.experimental import pallas as pl
from jax.experimental.pallas import tpu as pltpu
from jax.sharding import PartitionSpec as P

LEVELS = 3
ALPHA = -1.586134342059924
BETA = -0.052980118572961
GAMMA = 0.882911075530934
DELTA = 0.443506852043971
ZETA = 1.149604398860241
INVERSE_ZETA = 1.0 / 1.149604398860241
LANES = 128
EDGE = 8


def for_right(s_2, d_2, s_1, d_1):
    return d_1 + ALPHA * s_1, s_1 + BETA * (d_2 + ALPHA * (s_2 + s_1))


def for_left(s_0, d_0, s_1):
    return s_0, s_0 + BETA * (d_0 + ALPHA * (s_0 + s_1))


def lift(s, d, before, after, put):
    n = len(s)
    d1_last = before[0] + ALPHA * s[0]
    s1_last = before[1] + BETA * d1_last
    d2_last = None
    for i in range(n + 1):
        if i < n:
            s_next = s[i + 1] if i + 1 < n else after[0]
            d1 = d[i] + ALPHA * (s[i] + s_next)
            s1 = s[i] + BETA * (d1_last + d1)
        else:
            d1, s1 = None, after[1] + BETA * d1_last
        d2 = d1_last + GAMMA * (s1_last + s1)
        if i > 0:
            put(i - 1, (s1_last + DELTA * (d2_last + d2)) * ZETA, d2 * INVERSE_ZETA)
        d1_last, s1_last, d2_last = d1, s1, d2


def lifting_matrices(length):
    n = length // 2
    basis = np.eye(length + 4)
    s = [basis[2 * i] for i in range(n)]
    d = [basis[2 * i + 1] for i in range(n)]
    out = np.zeros((length + 4, length))

    def put(i, even, odd):
        out[:, 2 * i] = even
        out[:, 2 * i + 1] = odd

    rim = basis[length:]
    lift(s, d, (rim[0], rim[1]), (rim[2], rim[3]), put)
    return out[:length], out[length:]


def halves(a):
    high = a.astype(jnp.bfloat16)
    low = (a - high.astype(jnp.float32)).astype(jnp.bfloat16)
    return high, low


def np_halves(a):
    a = a.astype(np.float32)
    high = a.astype(jnp.bfloat16)
    low = (a - high.astype(np.float32)).astype(jnp.bfloat16)
    return high, low


class Sizes:
    def __init__(self, shape, step, valid):
        self.z, self.x, self.lanes = shape
        self.step = step
        self.y = valid
        self.out = max(LANES, -(-valid // LANES) * LANES)
        inner, rim = lifting_matrices(valid)
        full = np.zeros((self.lanes, self.out))
        full[: step * valid : step, :valid] = inner
        self.high, self.low = np_halves(full)
        edge = np.zeros((4, self.out))
        edge[:, :valid] = rim
        self.rim_high, self.rim_low = np_halves(edge)
        zeros = np.zeros((4, self.out), self.rim_high.dtype)
        self.rim_packed = np.concatenate([self.rim_high, self.rim_high, self.rim_low, zeros])


def dot(a, b):
    return jnp.dot(a, b, preferred_element_type=jnp.float32)


def times(rows, high_ref, low_ref):
    a, b = halves(rows)
    return dot(a, high_ref[...]) + dot(b, high_ref[...]) + dot(a, low_ref[...])


def whole(shape):
    return pl.BlockSpec(shape, lambda *_: (0,) * len(shape))


def edges_kernel(sizes, count, x_ref, left_ref, right_ref):
    step, n = sizes.step, sizes.y
    tile = (step * (n - 1)) // LANES * LANES
    low_lane = lax.broadcasted_iota(jnp.int32, (sizes.x, LANES), 1) < LANES // 2
    for p in range(count):
        both = x_ref[p, :, :LANES]
        if tile:
            both = jnp.where(low_lane, both, x_ref[p, :, tile : tile + LANES])
        both = both.T
        f = [both[step * k : step * k + 1] for k in range(3)]
        l = [both[step * (n - k) - tile : step * (n - k) - tile + 1] for k in (4, 3, 2, 1)]
        s, c = for_left(f[0], f[1], f[2])
        a, b = for_right(*l)
        left_ref[p, 0:1] = s
        left_ref[p, 1:2] = c
        right_ref[p, 0:1] = a
        right_ref[p, 1:2] = b


def edges(sizes, x):
    count = min(16, sizes.z)
    out = jax.ShapeDtypeStruct((sizes.z, 2, sizes.x), jnp.float32)
    spec = pl.BlockSpec((count, 2, sizes.x), lambda i: (i, 0, 0))
    return pl.pallas_call(
        functools.partial(edges_kernel, sizes, count),
        grid=(sizes.z // count,),
        in_specs=[pl.BlockSpec((count, sizes.x, sizes.lanes), lambda i: (i, 0, 0))],
        out_specs=[spec, spec],
        out_shape=[out, out],
        name="edges",
    )(x)


def rows_kernel(sizes, top_ref, bottom_ref, rim_rows_ref, high_ref, low_ref, rim_high_ref, rim_low_ref, left_ref, right_ref):
    z = sizes.z

    def across(ref, at):
        out = times(ref[...].reshape(z * 8, sizes.lanes), high_ref, low_ref)
        columns = rim_rows_ref[:, 8 * at : 8 * at + 8, :].reshape(z * 8, 4)
        return (out + times(columns, rim_high_ref, rim_low_ref)).reshape(z, 8, sizes.out)

    top = across(top_ref, 0)
    bottom = across(bottom_ref, 1)
    s, c = for_left(top[:, 0:1], top[:, 1:2], top[:, 2:3])
    a, b = for_right(bottom[:, 4:5], bottom[:, 5:6], bottom[:, 6:7], bottom[:, 7:8])
    left_ref[:, 0:1] = s
    left_ref[:, 1:2] = c
    right_ref[:, 0:1] = a
    right_ref[:, 1:2] = b


def rows(sizes, x, rim_rows):
    z = sizes.z
    out = jax.ShapeDtypeStruct((z, 2, sizes.out), jnp.float32)
    last = sizes.x // 8 - 1
    return pl.pallas_call(
        functools.partial(rows_kernel, sizes),
        grid=(1,),
        in_specs=[
            pl.BlockSpec((z, 8, sizes.lanes), lambda i: (0, 0, 0)),
            pl.BlockSpec((z, 8, sizes.lanes), lambda i: (0, last, 0)),
            whole(rim_rows.shape),
            whole(sizes.high.shape),
            whole(sizes.low.shape),
            whole(sizes.rim_high.shape),
            whole(sizes.rim_low.shape),
        ],
        out_specs=[whole(out.shape), whole(out.shape)],
        out_shape=[out, out],
        name="rows",
    )(x, x, rim_rows, sizes.high, sizes.low, sizes.rim_high, sizes.rim_low)


def across_planes(sizes, count, refs, work):
    x_ref, yb_ref, ya_ref, xb_ref, xa_ref, high_ref, low_ref, rim_ref = refs
    nx = sizes.x
    n = nx // 2
    for p in range(count):
        rim = jnp.concatenate([yb_ref[p], ya_ref[p]], axis=0)
        high = rim.astype(jnp.bfloat16).astype(jnp.float32)
        packed = jnp.concatenate([high, rim - high, high, jnp.zeros_like(high)], axis=0)
        across = times(x_ref[p], high_ref, low_ref) + dot(packed.T.astype(jnp.bfloat16), rim_ref[...])
        for c in range(sizes.out // LANES):
            lanes = slice(c * LANES, (c + 1) * LANES)

            def row(ref, k):
                return ref[p, k : k + 1, lanes]

            def at(start):
                return pl.ds(EDGE + start, n, stride=2)

            def one(k):
                return slice(EDGE + k, EDGE + k + 1)

            work[p, c, EDGE : EDGE + nx] = across[:, lanes]
            work[p, c, one(nx)] = row(xa_ref, 0)
            s = work[p, c, at(0)]
            d1 = work[p, c, at(1)] + ALPHA * (s + work[p, c, at(2)])
            d1_b = row(xb_ref, 0) + ALPHA * s[0:1]
            work[p, c, at(1)] = d1
            work[p, c, one(-1)] = d1_b
            s1 = s + BETA * (work[p, c, at(-1)] + d1)
            s1_b = row(xb_ref, 1) + BETA * d1_b
            work[p, c, at(0)] = s1
            work[p, c, one(nx)] = row(xa_ref, 1) + BETA * d1[n - 1 : n]
            d2 = d1 + GAMMA * (s1 + work[p, c, at(2)])
            work[p, c, at(1)] = d2
            work[p, c, one(-1)] = d1_b + GAMMA * (s1_b + s1[0:1])
            work[p, c, at(0)] = s1 + DELTA * (work[p, c, at(-1)] + d2)


def x_scale(height):
    even = lax.broadcasted_iota(jnp.int32, (height, LANES), 0) % 2 == 0
    return jnp.where(even, ZETA, INVERSE_ZETA).astype(jnp.float32)


def ends_kernel(sizes, *args):
    data, tables, out_ref, work, combined = args[:5], args[5:8], args[8], args[9], args[10:]

    def send(combine, picks, at):
        for ref, made in zip(data, combined):
            made[0], made[1] = combine(*[ref[k] for k in picks])
        across_planes(sizes, 2, (*combined, *tables), work)
        for k in range(2):
            for c in range(sizes.out // LANES):
                out_ref[at + k, :, c * LANES : (c + 1) * LANES] = work[k, c, EDGE : EDGE + sizes.x]

    pl.when(pl.program_id(0) == 0)(lambda: send(for_left, (0, 1, 2), 0))
    pl.when(pl.program_id(0) == 1)(lambda: send(for_right, (0, 1, 2, 3), 2))


def stream_kernel(sizes, group, steps, more, *args):
    refs, out_ref = args[:8], args[8]
    next_ref = args[9] if more else None
    work, state = args[-2:]
    step = pl.program_id(0)
    nx = sizes.x
    chunk = min(32, nx)
    even_scale = x_scale(chunk) * ZETA
    odd_scale = x_scale(chunk) * INVERSE_ZETA

    def take(pairs, slot):
        for c in range(sizes.out // LANES):
            lanes = slice(c * LANES, (c + 1) * LANES)
            for r in range(nx // chunk):
                at = slice(r * chunk, (r + 1) * chunk)
                held = slice(EDGE + r * chunk, EDGE + (r + 1) * chunk)
                s, d, d1_b, s1_b, d2_b = (state[k, c, at] for k in range(5))
                for q, pair in enumerate(pairs, slot):
                    s_n, d_n = work[2 * pair, c, held], work[2 * pair + 1, c, held]
                    d1 = d + ALPHA * (s + s_n)
                    s1 = s + BETA * (d1_b + d1)
                    d2 = d1_b + GAMMA * (s1_b + s1)
                    even = (s1_b + DELTA * (d2_b + d2)) * even_scale
                    out_ref[2 * q, at, lanes] = even
                    out_ref[2 * q + 1, at, lanes] = d2 * odd_scale
                    if more:
                        work[2 * pair, c, held] = even
                    s, d, d1_b, s1_b, d2_b = s_n, d_n, d1, s1, d2
                for k, v in enumerate((s, d, d1_b, s1_b, d2_b)):
                    state[k, c, at] = v
            if more:
                for q, pair in enumerate(pairs, slot):
                    next_ref[q, :, lanes] = work[2 * pair, c, pl.ds(EDGE, nx // 2, stride=2), :]

    late = range(2, group // 2)

    @pl.when(step == 0)
    def _():
        state[...] = jnp.zeros_like(state)
        work[...] = jnp.zeros_like(work)

    @pl.when(step < steps)
    def _():
        take(late, 0)
        across_planes(sizes, group, refs, work)

    @pl.when(step == steps)
    def _():
        take(late, 0)
        work[:4] = jnp.zeros((4,) + work.shape[1:], jnp.float32)

    take(range(2), len(late))


def across_specs(sizes, count, place):
    return [
        pl.BlockSpec((count, sizes.x, sizes.lanes), place),
        pl.BlockSpec((count, 2, sizes.x), place),
        pl.BlockSpec((count, 2, sizes.x), place),
        pl.BlockSpec((count, 2, sizes.out), place),
        pl.BlockSpec((count, 2, sizes.out), place),
        whole(sizes.high.shape),
        whole(sizes.low.shape),
        whole(sizes.rim_packed.shape),
    ]


def cost(sizes, count):
    return pl.CostEstimate(
        flops=count * sizes.x * sizes.out * sizes.lanes * 8,
        bytes_accessed=count * sizes.x * (sizes.out + sizes.lanes) * 4,
        transcendentals=0,
    )


def ends(sizes, *operands):
    out = jax.ShapeDtypeStruct((4, sizes.x, sizes.out), jnp.float32)
    last = sizes.z // 4 - 1
    return pl.pallas_call(
        functools.partial(ends_kernel, sizes),
        grid=(2,),
        in_specs=across_specs(sizes, 4, lambda i: (i * last, 0, 0)),
        out_specs=whole(out.shape),
        out_shape=out,
        scratch_shapes=[
            pltpu.VMEM((2, sizes.out // LANES, sizes.x + 2 * EDGE, LANES), jnp.float32),
            pltpu.VMEM((2, sizes.x, sizes.lanes), jnp.float32),
            pltpu.VMEM((2, 2, sizes.x), jnp.float32),
            pltpu.VMEM((2, 2, sizes.x), jnp.float32),
            pltpu.VMEM((2, 2, sizes.out), jnp.float32),
            pltpu.VMEM((2, 2, sizes.out), jnp.float32),
        ],
        cost_estimate=cost(sizes, 4),
        name="ends",
    )(*operands, sizes.high, sizes.low, sizes.rim_packed)


def stream(sizes, more, *operands):
    z, nx, width = sizes.z, sizes.x, sizes.out
    group = min(8, z)
    steps = z // group
    behind = lambda i: (jnp.maximum(i - 1, 0), 0, 0)
    out_shape = [jax.ShapeDtypeStruct((z, nx, width), jnp.float32)]
    out_specs = [pl.BlockSpec((group, nx, width), behind)]
    if more:
        out_shape.append(jax.ShapeDtypeStruct((z // 2, nx // 2, width), jnp.float32))
        out_specs.append(pl.BlockSpec((group // 2, nx // 2, width), behind))
    return pl.pallas_call(
        functools.partial(stream_kernel, sizes, group, steps, more),
        grid=(steps + 1,),
        in_specs=across_specs(sizes, group, lambda i: (jnp.minimum(i, steps - 1), 0, 0)),
        out_specs=out_specs,
        out_shape=out_shape,
        scratch_shapes=[
            pltpu.VMEM((group, width // LANES, nx + 2 * EDGE, LANES), jnp.float32),
            pltpu.VMEM((5, width // LANES, nx, LANES), jnp.float32),
        ],
        cost_estimate=cost(sizes, z),
        name="stream",
    )(*operands, sizes.high, sizes.low, sizes.rim_packed)


def finish_kernel(sizes, more, z_ref, t_ref, *rest):
    if more:
        _, out_ref, next_ref, work = rest
    else:
        out_ref = rest[0]
    nx = sizes.x
    rim = lifting_matrices(sizes.z)[1]
    single = sizes.z == 4
    scale = x_scale(nx)

    def apply(sides):
        for k in range(4):
            for c in range(sizes.out // LANES):
                lanes = slice(c * LANES, (c + 1) * LANES)
                total = jnp.zeros((nx, LANES), jnp.float32)
                for h in range(4):
                    factor = rim[h, k if h < 2 else sizes.z - 4 + k]
                    if factor != 0.0 and h // 2 in sides:
                        total = total + float(factor) * z_ref[(h + 2) % 4, :, lanes]
                total = t_ref[k, :, lanes] + scale * total
                out_ref[k, :, lanes] = total
                if more and k % 2 == 0:
                    work[c] = total
                    next_ref[k // 2, :, lanes] = work[c, pl.ds(0, nx // 2, stride=2), :]

    if single:
        apply((0, 1))
    else:
        pl.when(pl.program_id(0) == 0)(lambda: apply((0,)))
        pl.when(pl.program_id(0) == 1)(lambda: apply((1,)))


def finish(sizes, made, z_planes):
    more = len(made) == 2
    z, nx, width = sizes.z, sizes.x, sizes.out
    last = z // 4 - 1
    place = lambda i: (i * last, 0, 0)
    specs = [pl.BlockSpec((4, nx, width), place)]
    scratch = []
    if more:
        specs.append(pl.BlockSpec((2, nx // 2, width), place))
        scratch.append(pltpu.VMEM((width // LANES, nx, LANES), jnp.float32))
    return pl.pallas_call(
        functools.partial(finish_kernel, sizes, more),
        grid=(min(2, last + 1),),
        in_specs=[whole((4, nx, width))] + specs,
        out_specs=specs,
        out_shape=[jax.ShapeDtypeStruct(m.shape, m.dtype) for m in made],
        input_output_aliases={1 + k: k for k in range(len(made))},
        scratch_shapes=scratch,
        name="finish",
    )(z_planes, *made)


def spread_lanes(rows, table):
    high = rows.astype(jnp.bfloat16)
    middle, low = halves(rows - high.astype(jnp.float32))
    return dot(high, table) + dot(middle, table) + dot(low, table)


def put_inner(plane, inner, table, work):
    nx, width = plane.shape
    n = nx // 2
    even_lane = lax.broadcasted_iota(jnp.int32, (n, LANES), 1) % 2 == 0
    spread = spread_lanes(inner, table)
    for c in range(width // LANES):
        lanes = slice(c * LANES, (c + 1) * LANES)
        work[c] = plane[:, lanes]
        even_rows = work[c, pl.ds(0, n, stride=2), :]
        work[c, pl.ds(0, n, stride=2), :] = jnp.where(even_lane, spread[:, lanes], even_rows)


def place_kernel(count, t_ref, middle_ref, inner_ref, outer_table_ref, inner_table_ref, out_ref, work, inner_work):
    width, middle_width = t_ref.shape[3], middle_ref.shape[2]
    for p in range(count):
        middle = middle_ref[p]
        if p % 2 == 0:
            put_inner(middle, inner_ref[p // 2], inner_table_ref[...], inner_work)
            middle = jnp.concatenate([inner_work[c] for c in range(middle_width // LANES)], axis=1)
        put_inner(t_ref[p, 0], middle, outer_table_ref[...], work)
        for c in range(width // LANES):
            out_ref[p, 0, :, c * LANES : (c + 1) * LANES] = work[c]


def spread_table(inner, outer):
    table = np.zeros((inner, outer), np.float32)
    for j in range(min(inner, outer // 2)):
        table[j, 2 * j] = 1.0
    return table.astype(jnp.bfloat16)


def place(t, middle, inner):
    z, nx, width = t.shape
    tables = spread_table(middle.shape[2], width), spread_table(inner.shape[2], middle.shape[2])
    count = min(8, z // 2)
    spec = pl.BlockSpec((count, 1, nx, width), lambda i: (i, 0, 0, 0))
    paired = t.reshape(z // 2, 2, nx, width)
    return pl.pallas_call(
        functools.partial(place_kernel, count),
        grid=(z // 2 // count,),
        in_specs=[
            spec,
            pl.BlockSpec((count,) + middle.shape[1:], lambda i: (i, 0, 0)),
            pl.BlockSpec((count // 2,) + inner.shape[1:], lambda i: (i, 0, 0)),
            whole(tables[0].shape),
            whole(tables[1].shape),
        ],
        out_specs=spec,
        out_shape=jax.ShapeDtypeStruct(paired.shape, jnp.float32),
        input_output_aliases={0: 0},
        scratch_shapes=[
            pltpu.VMEM((width // LANES, nx, LANES), jnp.float32),
            pltpu.VMEM((middle.shape[2] // LANES,) + middle.shape[1:2] + (LANES,), jnp.float32),
        ],
        name="place",
    )(paired, middle, inner, *tables).reshape(t.shape)


def exchange(axis, left, right):
    count = lax.axis_size(axis)
    before = lax.ppermute(right, axis, [(i, (i + 1) % count) for i in range(count)])
    after = lax.ppermute(left, axis, [(i, (i - 1) % count) for i in range(count)])
    return before, after


def exchange_z(planes):
    count = lax.axis_size("gz")
    if count == 2:
        return lax.ppermute(planes, "gz", [(0, 1), (1, 0)])
    before, after = exchange("gz", planes[:2], planes[2:])
    return jnp.concatenate([after, before])


def level(sizes, x, more):
    y_before, y_after = exchange("gy", *edges(sizes, x))
    rim = jnp.concatenate([y_before, y_after], axis=1)
    rim_rows = jnp.concatenate([rim[:, :, :8], rim[:, :, -8:]], axis=2).swapaxes(1, 2)
    x_before, x_after = exchange("gx", *rows(sizes, x, rim_rows))
    operands = (x, y_before, y_after, x_before, x_after)
    z_planes = exchange_z(ends(sizes, *operands))
    return finish(sizes, stream(sizes, more, *operands), z_planes)


def local(turbulence):
    valid = turbulence.shape[2]
    current, step, done = turbulence, 1, []
    for index in range(LEVELS):
        more = index + 1 < LEVELS
        sizes = Sizes(current.shape, step, valid)
        made = level(sizes, current, more)
        done.append(made[0])
        if more:
            current, step, valid = made[1], 2, valid // 2
    return place(*done)[:, :, : turbulence.shape[2]]


def solution(mesh):
    spec = P("gz", "gx", "gy")
    return jax.shard_map(local, mesh=mesh, in_specs=(spec,), out_specs=spec, check_vma=False)
```
